32 devices in a mesh: ctx: 16 (over z, x, core), head: 2 (over y).
Axes of the slice: x: 2, y: 2, z: 4, core: 2. Of those that a mesh axis runs over, the one named last changes fastest.
Arguments:
- query_heads: bfloat16 [4096, 32, 128], P('ctx', 'head'), may hold values from -5 to 5
- key_heads: bfloat16 [4096, 16, 128], P('ctx', 'head'), may hold values from -5 to 5
- value_heads: bfloat16 [4096, 16, 128], P('ctx', 'head'), may hold values from -6 to 6
- positions: int32 [4096], P('ctx'), may hold values from 0 to 4095, each once
- out_weight: bfloat16 [4096, 4608], P('head'), may hold values from -0.125 to 0.125
Outputs:
- attn_out: bfloat16 [4096, 4608], P('ctx', 'head')
The draws below stay inside these ranges and needn't reach their ends.
Inputs may be any that keep to these rules, and one draw needn't show every extreme that they name: Each of the 4096 positions appears exactly once.
All inputs are finite; a program needn't handle non-finite values.
Results may differ from the reference program's by a relative error of at most 0.0081.
Values may be sent and summed in bfloat16 or wider, within the bound.
A program may use at most 64 MiB of HBM per device.

```python
import jax
import jax.numpy as jnp
from jax import lax

D = 4608
HEADS = 32
KV = 16
HD = 128
SEQ = 4096


def base_values(key, shape, spread):
    values = jax.random.normal(jax.random.fold_in(key, 5), shape, jnp.float32) * spread
    return jnp.clip(values, -5.0, 5.0)


def draw_query_heads(key, part):
    values = base_values(jax.random.fold_in(key, 1), (SEQ, HEADS, HD), 1.5)
    return values.astype(jnp.bfloat16)


def draw_key_heads(key, part):
    values = base_values(jax.random.fold_in(key, 2), (SEQ, KV, HD), 1.0)
    return values.astype(jnp.bfloat16)


def with_spikes(result, stream_key, source, target, blocks, factor):
    owner, partner = [(jnp.arange(result.shape[axis_at]) // (result.shape[axis_at] // blocks)).reshape([-1 if axis == axis_at else 1 for axis in range(result.ndim)]) for axis_at in (source, target)]
    chosen = jax.random.permutation(stream_key, blocks)[partner]
    strong = (owner == chosen) | (owner == (partner + blocks // 2) % blocks)
    return jnp.where(strong, factor * result, result)


def shard_levels(stream_key, extent, shards, least, top_value):
    factor_of, own = 1.0, jax.random.fold_in(stream_key, 6)
    for dim, blocks in shards:
        draws = jnp.exp(jax.random.uniform(jax.random.fold_in(own, dim), (blocks,), jnp.float32, least / len(shards), top_value / len(shards)))
        factor_of = factor_of * jnp.repeat(draws, extent[dim] // blocks).reshape([-1 if axis == dim else 1 for axis in range(len(extent))])
    return factor_of


def normal_values(stream_key, shape, scale, bound, pieces=(), kind=jnp.bfloat16):
    array = jax.random.normal(stream_key, shape, jnp.float32) * scale
    if len(pieces) > 0:
        array = shard_levels(stream_key, shape, pieces, -0.22, 0.18) * array
    return jnp.clip(array, min=-bound, max=bound).astype(kind)


def bell_draw_with(own_key, shape, scale, reach, pieces, heavy, held_as=jnp.bfloat16):
    result = scale * jax.random.normal(own_key, shape, jnp.float32)
    if pieces:
        result = result * shard_levels(own_key, shape, pieces, -0.22, 0.18)
    return jnp.clip(with_spikes(result, jax.random.fold_in(own_key, 3), *heavy), -reach, reach).astype(held_as)


def setup_inputs(seed: int = 0) -> dict:
    arg_keys = jax.random.split(jax.random.key(seed), 6)
    query_heads = draw_query_heads(jax.random.fold_in(arg_keys[5], 71), 0)
    key_heads = draw_key_heads(jax.random.fold_in(arg_keys[5], 71), 0)
    value_heads = normal_values(arg_keys[2], (SEQ, KV, HD), 1.0, 6.0, ((0, 16), (1, 2)))
    positions = jax.random.permutation(arg_keys[3], SEQ).astype(jnp.int32)
    out_weight = bell_draw_with(arg_keys[4], (HEADS * HD, D), (HEADS * HD) ** -0.5, 0.125, ((0, 2),), (0, 1, 2, 2.0))
    return dict(query_heads=query_heads, key_heads=key_heads, value_heads=value_heads, positions=positions, out_weight=out_weight)


NEG_BIG = -1.0e30
ATTN_SCALE = 1.0 / 12.0


def reference(query_heads, key_heads, value_heads, positions, out_weight):
    group_size = HEADS // KV
    visible = positions[None, :] <= positions[:, None]

    def one_head(head_index):
        query_one = lax.dynamic_index_in_dim(query_heads, head_index, 1, keepdims=False)
        kv_index = (head_index // group_size).astype(jnp.int32)
        key_one = lax.dynamic_index_in_dim(key_heads, kv_index, 1, keepdims=False)
        value_one = lax.dynamic_index_in_dim(value_heads, kv_index, 1, keepdims=False)
        scores = jnp.dot(query_one, key_one.T, preferred_element_type=jnp.float32) * ATTN_SCALE
        scores = jnp.where(visible, scores, NEG_BIG)
        row_max = jnp.max(scores, axis=1)
        weights = jnp.where(visible, jnp.exp(scores - row_max[:, None]), 0.0)
        denom = jnp.sum(weights, axis=1)
        summed = jnp.dot(weights.astype(jnp.bfloat16), value_one, preferred_element_type=jnp.float32)
        return (summed / denom[:, None]).astype(jnp.bfloat16)

    attended = lax.map(one_head, jnp.arange(HEADS, dtype=jnp.int32))
    flat = jnp.transpose(attended, (1, 0, 2)).reshape(SEQ, HEADS * HD)
    return jnp.dot(flat, out_weight, preferred_element_type=jnp.float32).astype(jnp.bfloat16)
```

```python
import functools
import math

import jax
import jax.numpy as jnp
from jax import lax
from jax.experimental import pallas as pl
from jax.experimental.pallas import tpu as pltpu
from jax.sharding import PartitionSpec as P

NEG_BIG = -1e30
ATTN_SCALE = 1.0 / 12.0
EXP2_SCALE = ATTN_SCALE * math.log2(math.e)
MESH = pl.DeviceIdType.MESH
QUAD = 4


def plain_on_device(query_heads, key_heads, value_heads, positions, out_weight):
    tok_local, heads_local, head_size = query_heads.shape
    kv_local = key_heads.shape[1]
    group_size = heads_local // kv_local
    grouped = query_heads.reshape(tok_local, kv_local, group_size, head_size)
    all_positions = lax.all_gather(positions, "ctx", axis=0, tiled=True)
    stat_shape = (kv_local, group_size, tok_local)
    initial = (
        jnp.full(stat_shape, NEG_BIG, jnp.float32),
        jnp.zeros(stat_shape, jnp.float32),
        jnp.zeros(stat_shape + (head_size,), jnp.float32),
    )

    def attend_block(carry, key_block, value_block, key_pos):
        running_max, running_sum, accum = carry
        scores = (
            jnp.einsum("tkgd,skd->kgts", grouped, key_block, preferred_element_type=jnp.float32)
            * ATTN_SCALE
        )
        visible = key_pos[None, :] <= positions[:, None]
        scores = jnp.where(visible, scores, NEG_BIG)
        new_max = jnp.maximum(running_max, jnp.max(scores, axis=-1))
        weights = jnp.where(visible, jnp.exp(scores - new_max[..., None]), 0.0)
        decay_old = jnp.exp(running_max - new_max)
        running_sum = running_sum * decay_old + jnp.sum(weights, axis=-1)
        accum = accum * decay_old[..., None] + jnp.einsum(
            "kgts,skd->kgtd",
            weights.astype(jnp.bfloat16),
            value_block,
            preferred_element_type=jnp.float32,
        )
        return (new_max, running_sum, accum)

    key_all, value_all = (
        lax.all_gather(key_heads, "ctx", axis=0, tiled=True),
        lax.all_gather(value_heads, "ctx", axis=0, tiled=True),
    )
    piece_rows = key_all.shape[0]
    block_rows = math.gcd(piece_rows, 1024)

    def one_block(inner, block_index):
        offset = block_index * block_rows
        key_block = lax.dynamic_slice_in_dim(key_all, offset, block_rows, 0)
        value_block = lax.dynamic_slice_in_dim(value_all, offset, block_rows, 0)
        key_pos = lax.dynamic_slice_in_dim(all_positions, offset, block_rows, 0)
        return (attend_block(inner, key_block, value_block, key_pos), None)

    result, _ = lax.scan(one_block, initial, jnp.arange(piece_rows // block_rows, dtype=jnp.int32))
    _, total, accum = result
    attended = (accum / total[..., None]).astype(jnp.bfloat16)
    flat = jnp.transpose(attended, (2, 0, 1, 3)).reshape(tok_local, heads_local * head_size)
    terms = jnp.dot(flat, out_weight, preferred_element_type=jnp.float32)
    return lax.psum_scatter(terms, "head", scatter_dimension=1, tiled=True).astype(jnp.bfloat16)


def fused_kernel(
    n_ctx, n_blocks, q_in, kv_in, pos_in, w_hbm, out_ref,
    kvbuf, qbuf, posbuf, qcol, m_ref, acc_ref, obuf, attbuf, w_vmem, sendbuf, recvbuf, ownbuf,
    w_sem, pos_send, pos_recv, kvq_send, kvq_recv, q_send, q_recv,
    up_send, down_send, below_recv, above_recv, att_send, att_recv, y_send, y_recv,
):
    me = lax.axis_index("ctx")
    head = lax.axis_index("head")
    nz = n_ctx // QUAD
    z = me // QUAD
    s = me % QUAD
    s_hi, s_lo = s // 2, s % 2
    n_kv, _, tok, hd = kv_in.shape
    groups = n_kv // QUAD
    rep = q_in.shape[0] // n_kv
    tok_z = QUAD * tok
    half = out_ref.shape[1]
    width = half // n_blocks

    def peer(d):
        hi = s_hi if d < 2 else 1 - s_hi
        lo = s_lo if d % 2 == 0 else 1 - s_lo
        return 2 * hi + lo

    def rows(idx):
        return pl.ds(pl.multiple_of(idx * tok, tok), tok)

    barrier = pltpu.get_barrier_semaphore()
    for d in range(1, n_ctx):
        pl.semaphore_signal(
            barrier, inc=1, device_id=(lax.rem(me + d, n_ctx), head), device_id_type=MESH
        )
    pl.semaphore_signal(barrier, inc=1, device_id=(me, 1 - head), device_id_type=MESH)
    pl.semaphore_wait(barrier, n_ctx)

    def remote(src, dst, ssem, rsem, ctx, hh=None):
        return pltpu.make_async_remote_copy(
            src_ref=src, dst_ref=dst, send_sem=ssem, recv_sem=rsem,
            device_id=(ctx, head if hh is None else hh), device_id_type=MESH,
        )

    def pos_copy(d):
        return remote(
            pos_in, posbuf.at[me], pos_send.at[d], pos_recv.at[d], lax.rem(me + d, n_ctx)
        )

    def kv_copy(d, g):
        p = peer(d)
        return remote(
            kv_in.at[p * groups + g], kvbuf.at[z, g, :, rows(s), :],
            kvq_send.at[d, g], kvq_recv.at[d, g], z * QUAD + p,
        )

    def q_copy(d, g):
        p = peer(d)
        return remote(
            q_in.at[pl.ds((p * groups + g) * rep, rep)],
            qbuf.at[pl.ds(g * rep, rep), rows(s), :],
            q_send.at[d, g], q_recv.at[d, g], z * QUAD + p,
        )

    def z_send_part(g, src, idx):
        dst = kvbuf.at[z, g, :, rows(idx), :]

        @pl.when(z > 0)
        def _():
            remote(src, dst, down_send.at[0, g], above_recv.at[1, g], me - QUAD).start()

        @pl.when(z < nz - 1)
        def _():
            remote(src, dst, up_send.at[0, g], below_recv.at[1, g], me + QUAD).start()

    def down_chunk(k, g):
        chunk = kvbuf.at[z + k, g]
        return remote(chunk, chunk, down_send.at[k, g], above_recv.at[k + 1, g], me - QUAD)

    def up_chunk(k, g):
        chunk = kvbuf.at[z - k, g]
        return remote(chunk, chunk, up_send.at[k, g], below_recv.at[k + 1, g], me + QUAD)

    def wait_above(k, g):
        chunk = kvbuf.at[z + k, g]
        remote(chunk, chunk, down_send.at[k, g], above_recv.at[k, g], me).wait_recv()

    def wait_below(k, g):
        chunk = kvbuf.at[z - k, g]
        remote(chunk, chunk, up_send.at[k, g], below_recv.at[k, g], me).wait_recv()

    for g in range(groups):
        for d in (1, 2, 3):
            kv_copy(d, g).start()
        if g == 0:
            for d in range(1, n_ctx):
                pos_copy(d).start()
        z_send_part(g, kv_in.at[s * groups + g], s)
        for d in (1, 2, 3):
            q_copy(d, g).start()
    w_copies = []
    for part in range(2):
        col = (1 - head) if part == 0 else head
        w_copies.append(
            pltpu.make_async_copy(
                w_hbm.at[:, pl.ds(pl.multiple_of(col * half, 128), half)],
                w_vmem.at[part], w_sem.at[part],
            )
        )
        w_copies[-1].start()

    posbuf[me] = pos_in[...]
    for g in range(groups):
        kvbuf[z, g, :, rows(s), :] = kv_in[s * groups + g]
        for r in range(rep):
            qbuf[g * rep + r, rows(s), :] = q_in[(s * groups + g) * rep + r]
    m_ref[...] = jnp.full(m_ref.shape, NEG_BIG, jnp.float32)
    acc_ref[...] = jnp.zeros(acc_ref.shape, jnp.float32)

    def own_parts(g):
        for d in (1, 2, 3):
            kv_copy(d, g).wait_recv()
            p = peer(d)
            z_send_part(g, kvbuf.at[z, g, :, rows(p), :], p)

    def compute(layer, g):
        key_pos = jnp.concatenate([posbuf[layer * QUAD + i] for i in range(QUAD)], axis=1)
        key_pos = key_pos.astype(jnp.float32)

        def tile(i, _):
            r = i // QUAD
            t = i % QUAD
            q = qbuf[g * rep + r, rows(t), :]
            keys = kvbuf[layer, g, 0]
            values = kvbuf[layer, g, 1]
            x = lax.dot_general(
                q, keys, (((1,), (1,)), ((), ())), preferred_element_type=jnp.float32
            ) * EXP2_SCALE
            q_pos = qcol[rows(t), :][:, :1]
            x = jnp.where(key_pos <= q_pos, x, NEG_BIG)
            m_old = m_ref[g * rep + r, rows(t), :]
            m_new = jnp.maximum(m_old, jnp.max(x, axis=1, keepdims=True))
            m_ref[g * rep + r, rows(t), :] = m_new
            decay = jnp.exp2(m_old - m_new)
            weights = jnp.exp2(x - m_new[:, :1]).astype(jnp.bfloat16)
            extended = jnp.concatenate([values, jnp.ones_like(values)], axis=1)
            new = jnp.dot(weights, extended, preferred_element_type=jnp.float32)
            old = acc_ref[g * rep + r, rows(t), :]
            acc_ref[g * rep + r, rows(t), :] = (
                old * jnp.concatenate([decay, decay], axis=1) + new
            )
            return 0

        lax.fori_loop(0, rep * QUAD, tile, 0)

    def att_copy(d, g):
        p = peer(d)
        cols = pl.ds(g * rep * hd, rep * hd)
        return remote(
            obuf.at[rows(p), cols], attbuf.at[s, :, cols],
            att_send.at[d, g], att_recv.at[d, g], z * QUAD + p,
        )

    def finish(g):
        for r in range(rep):
            for t in range(QUAD):
                part = acc_ref[g * rep + r, t * tok:(t + 1) * tok, :]
                done = (part[:, :hd] / part[:, hd:]).astype(jnp.bfloat16)
                obuf[t * tok:(t + 1) * tok, (g * rep + r) * hd:(g * rep + r + 1) * hd] = done
        for d in (3, 2, 1):
            att_copy(d, g).start()
        cols = slice(g * rep * hd, (g + 1) * rep * hd)
        attbuf[s, :, cols] = obuf[rows(s), cols]

    for g in range(groups):
        own_parts(g)
        if g == 0:
            for d in range(1, n_ctx):
                pos_copy(d).wait_recv()
            for i in range(QUAD):
                line = posbuf[z * QUAD + i].astype(jnp.float32)
                for j in range(tok // 128):
                    piece = jnp.broadcast_to(line[:, j * 128:(j + 1) * 128], (128, 128))
                    qcol[i * tok + j * 128:i * tok + (j + 1) * 128, :] = piece.T
        for d in (1, 2, 3):
            q_copy(d, g).wait_recv()
        compute(z, g)

    for k in range(1, nz):
        for g in range(groups):
            @pl.when(z + k < nz)
            def _():
                wait_above(k, g)

                @pl.when(z > 0)
                def _():
                    down_chunk(k, g).start()

                compute(z + k, g)

            @pl.when(z - k >= 0)
            def _():
                wait_below(k, g)

                @pl.when(z < nz - 1)
                def _():
                    up_chunk(k, g).start()

                compute(z - k, g)

            if k == nz - 1:
                finish(g)
    if nz == 1:
        for g in range(groups):
            finish(g)

    def y_copy(b):
        return remote(
            sendbuf.at[b], recvbuf.at[b], y_send.at[b], y_recv.at[b], me, 1 - head
        )

    for g in range(groups):
        for d in (1, 2, 3):
            att_copy(d, g).wait_recv()

    def product(part, b):
        total = None
        depth = groups * rep * hd
        for j in range(QUAD):
            term = jnp.dot(
                attbuf[j],
                w_vmem[part, j * depth:(j + 1) * depth, b * width:(b + 1) * width],
                preferred_element_type=jnp.float32,
            )
            total = term if total is None else total + term
        return total

    w_copies[0].wait()
    for b in range(n_blocks):
        sendbuf[b] = product(0, b).astype(jnp.bfloat16)
        y_copy(b).start()
    w_copies[1].wait()
    for b in range(n_blocks):
        ownbuf[b] = product(1, b)
    for b in range(n_blocks):
        y_copy(b).wait_recv()
        out_ref[:, b * width:(b + 1) * width] = (
            ownbuf[b] + recvbuf[b].astype(jnp.float32)
        ).astype(jnp.bfloat16)

    for d in range(1, n_ctx):
        pos_copy(d).wait_send()
    for g in range(groups):
        for d in (1, 2, 3):
            kv_copy(d, g).wait_send()
            q_copy(d, g).wait_send()
            att_copy(d, g).wait_send()
        for k in range(nz - 1):
            @pl.when((z > 0) & (z + k < nz))
            def _():
                down_chunk(k, g).wait_send()

            @pl.when((z < nz - 1) & (z - k >= 0))
            def _():
                up_chunk(k, g).wait_send()
    for b in range(n_blocks):
        y_copy(b).wait_send()


def fused_on_device(n_ctx, query_heads, key_heads, value_heads, positions, out_weight):
    tok, n_q, hd = query_heads.shape
    n_kv = key_heads.shape[1]
    q = jnp.transpose(query_heads, (1, 0, 2))
    kv = jnp.transpose(jnp.stack([key_heads, value_heads]), (2, 0, 1, 3))
    pos = positions.reshape(1, tok)
    nz = n_ctx // QUAD
    groups = n_kv // QUAD
    q_dev = n_q // QUAD
    tok_z = QUAD * tok
    rows_w, model = out_weight.shape
    half = model // 2
    n_blocks = 3 if half % 384 == 0 else 1
    width = half // n_blocks
    vmem = pltpu.VMEM
    dma = pltpu.SemaphoreType.DMA
    whole = pl.BlockSpec(memory_space=pltpu.VMEM)
    return pl.pallas_call(
        functools.partial(fused_kernel, n_ctx, n_blocks),
        out_shape=jax.ShapeDtypeStruct((tok, half), jnp.bfloat16),
        in_specs=[whole, whole, whole, pl.BlockSpec(memory_space=pl.ANY)],
        out_specs=whole,
        scratch_shapes=[
            vmem((nz, groups, 2, tok_z, hd), jnp.bfloat16),
            vmem((q_dev, tok_z, hd), jnp.bfloat16),
            vmem((n_ctx, 1, tok), jnp.int32),
            vmem((tok_z, 128), jnp.float32),
            vmem((q_dev, tok_z, hd), jnp.float32),
            vmem((q_dev, tok_z, 2 * hd), jnp.float32),
            vmem((tok_z, q_dev * hd), jnp.bfloat16),
            vmem((QUAD, tok, q_dev * hd), jnp.bfloat16),
            vmem((2, rows_w, half), jnp.bfloat16),
            vmem((n_blocks, tok, width), jnp.bfloat16),
            vmem((n_blocks, tok, width), jnp.bfloat16),
            vmem((n_blocks, tok, width), jnp.float32),
            dma((2,)),
            dma((n_ctx,)), dma((n_ctx,)),
            dma((QUAD, groups)), dma((QUAD, groups)),
            dma((QUAD, groups)), dma((QUAD, groups)),
            dma((nz, groups)), dma((nz, groups)),
            dma((nz + 1, groups)), dma((nz + 1, groups)),
            dma((QUAD, groups)), dma((QUAD, groups)),
            dma((n_blocks,)), dma((n_blocks,)),
        ],
        compiler_params=pltpu.CompilerParams(
            collective_id=0, has_side_effects=True, vmem_limit_bytes=62 * 1024 * 1024
        ),
    )(q, kv, pos, out_weight)


def solution(mesh):
    placed = (
        P("ctx", "head", None),
        P("ctx", "head", None),
        P("ctx", "head", None),
        P("ctx"),
        P("head", None),
    )
    n_ctx, n_head = mesh.shape["ctx"], mesh.shape["head"]

    def on_device(query_heads, key_heads, value_heads, positions, out_weight):
        args = (query_heads, key_heads, value_heads, positions, out_weight)
        fits = (
            n_head == 2 and n_ctx % QUAD == 0 and key_heads.shape[1] % QUAD == 0
            and query_heads.shape[2] == 128 and query_heads.shape[0] % 128 == 0
            and out_weight.shape[1] % 256 == 0
        )
        if fits:
            return fused_on_device(n_ctx, *args)
        return plain_on_device(*args)

    return jax.shard_map(
        on_device, mesh=mesh, in_specs=placed, out_specs=P("ctx", "head"), check_vma=False
    )
```

```python
import functools
import math

import jax
import jax.numpy as jnp
from jax import lax
from jax.experimental import pallas as pl
from jax.experimental.pallas import tpu as pltpu
from jax.sharding import PartitionSpec as P

NEG_BIG = -1e30
ATTN_SCALE = 1.0 / 12.0
EXP2_SCALE = ATTN_SCALE * math.log2(math.e)
MESH = pl.DeviceIdType.MESH
QUAD = 4


def plain_on_device(query_heads, key_heads, value_heads, positions, out_weight):
    tok_local, heads_local, head_size = query_heads.shape
    kv_local = key_heads.shape[1]
    group_size = heads_local // kv_local
    grouped = query_heads.reshape(tok_local, kv_local, group_size, head_size)
    all_positions = lax.all_gather(positions, "ctx", axis=0, tiled=True)
    stat_shape = (kv_local, group_size, tok_local)
    initial = (
        jnp.full(stat_shape, NEG_BIG, jnp.float32),
        jnp.zeros(stat_shape, jnp.float32),
        jnp.zeros(stat_shape + (head_size,), jnp.float32),
    )

    def attend_block(carry, key_block, value_block, key_pos):
        running_max, running_sum, accum = carry
        scores = (
            jnp.einsum("tkgd,skd->kgts", grouped, key_block, preferred_element_type=jnp.float32)
            * ATTN_SCALE
        )
        visible = key_pos[None, :] <= positions[:, None]
        scores = jnp.where(visible, scores, NEG_BIG)
        new_max = jnp.maximum(running_max, jnp.max(scores, axis=-1))
        weights = jnp.where(visible, jnp.exp(scores - new_max[..., None]), 0.0)
        decay_old = jnp.exp(running_max - new_max)
        running_sum = running_sum * decay_old + jnp.sum(weights, axis=-1)
        accum = accum * decay_old[..., None] + jnp.einsum(
            "kgts,skd->kgtd",
            weights.astype(jnp.bfloat16),
            value_block,
            preferred_element_type=jnp.float32,
        )
        return (new_max, running_sum, accum)

    key_all, value_all = (
        lax.all_gather(key_heads, "ctx", axis=0, tiled=True),
        lax.all_gather(value_heads, "ctx", axis=0, tiled=True),
    )
    piece_rows = key_all.shape[0]
    block_rows = math.gcd(piece_rows, 1024)

    def one_block(inner, block_index):
        offset = block_index * block_rows
        key_block = lax.dynamic_slice_in_dim(key_all, offset, block_rows, 0)
        value_block = lax.dynamic_slice_in_dim(value_all, offset, block_rows, 0)
        key_pos = lax.dynamic_slice_in_dim(all_positions, offset, block_rows, 0)
        return (attend_block(inner, key_block, value_block, key_pos), None)

    result, _ = lax.scan(one_block, initial, jnp.arange(piece_rows // block_rows, dtype=jnp.int32))
    _, total, accum = result
    attended = (accum / total[..., None]).astype(jnp.bfloat16)
    flat = jnp.transpose(attended, (2, 0, 1, 3)).reshape(tok_local, heads_local * head_size)
    terms = jnp.dot(flat, out_weight, preferred_element_type=jnp.float32)
    return lax.psum_scatter(terms, "head", scatter_dimension=1, tiled=True).astype(jnp.bfloat16)


def fused_kernel(
    n_ctx, n_blocks, q_in, kv_in, pos_in, w_hbm, out_ref,
    kvbuf, qbuf, posbuf, qcol, m_ref, acc_ref, obuf, attbuf, w_vmem, sendbuf, recvbuf, ownbuf, key_t,
    w_sem, pos_send, pos_recv, kvq_send, kvq_recv, q_send, q_recv,
    up_send, down_send, below_recv, above_recv, att_send, att_recv, y_send, y_recv,
):
    me = lax.axis_index("ctx")
    head = lax.axis_index("head")
    nz = n_ctx // QUAD
    z = me // QUAD
    s = me % QUAD
    s_hi, s_lo = s // 2, s % 2
    n_kv, _, tok, hd = kv_in.shape
    groups = n_kv // QUAD
    rep = q_in.shape[0] // n_kv
    tok_z = QUAD * tok
    half = out_ref.shape[1]
    width = half // n_blocks

    def peer(d):
        hi = s_hi if d < 2 else 1 - s_hi
        lo = s_lo if d % 2 == 0 else 1 - s_lo
        return 2 * hi + lo

    def rows(idx):
        return pl.ds(pl.multiple_of(idx * tok, tok), tok)

    barrier = pltpu.get_barrier_semaphore()
    for d in range(1, n_ctx):
        pl.semaphore_signal(
            barrier, inc=1, device_id=(lax.rem(me + d, n_ctx), head), device_id_type=MESH
        )
    pl.semaphore_signal(barrier, inc=1, device_id=(me, 1 - head), device_id_type=MESH)
    pl.semaphore_wait(barrier, n_ctx)

    def remote(src, dst, ssem, rsem, ctx, hh=None):
        return pltpu.make_async_remote_copy(
            src_ref=src, dst_ref=dst, send_sem=ssem, recv_sem=rsem,
            device_id=(ctx, head if hh is None else hh), device_id_type=MESH,
        )

    def pos_copy(d):
        return remote(
            pos_in, posbuf.at[me], pos_send.at[d], pos_recv.at[d], lax.rem(me + d, n_ctx)
        )

    def kv_copy(d, g):
        p = peer(d)
        return remote(
            kv_in.at[p * groups + g], kvbuf.at[z, g, :, rows(s), :],
            kvq_send.at[d, g], kvq_recv.at[d, g], z * QUAD + p,
        )

    def q_copy(d, g):
        p = peer(d)
        return remote(
            q_in.at[pl.ds((p * groups + g) * rep, rep)],
            qbuf.at[pl.ds(g * rep, rep), rows(s), :],
            q_send.at[d, g], q_recv.at[d, g], z * QUAD + p,
        )

    def z_send_part(g, src, idx):
        dst = kvbuf.at[z, g, :, rows(idx), :]

        @pl.when(z > 0)
        def _():
            remote(src, dst, down_send.at[0, g], above_recv.at[1, g], me - QUAD).start()

        @pl.when(z < nz - 1)
        def _():
            remote(src, dst, up_send.at[0, g], below_recv.at[1, g], me + QUAD).start()

    def down_chunk(k, g):
        chunk = kvbuf.at[z + k, g]
        return remote(chunk, chunk, down_send.at[k, g], above_recv.at[k + 1, g], me - QUAD)

    def up_chunk(k, g):
        chunk = kvbuf.at[z - k, g]
        return remote(chunk, chunk, up_send.at[k, g], below_recv.at[k + 1, g], me + QUAD)

    def wait_above(k, g):
        chunk = kvbuf.at[z + k, g]
        remote(chunk, chunk, down_send.at[k, g], above_recv.at[k, g], me).wait_recv()

    def wait_below(k, g):
        chunk = kvbuf.at[z - k, g]
        remote(chunk, chunk, up_send.at[k, g], below_recv.at[k, g], me).wait_recv()

    for g in range(groups):
        for d in (1, 2, 3):
            kv_copy(d, g).start()
        if g == 0:
            for d in range(1, n_ctx):
                pos_copy(d).start()
        z_send_part(g, kv_in.at[s * groups + g], s)
        for d in (1, 2, 3):
            q_copy(d, g).start()
    w_copies = []
    for part in range(2):
        col = (1 - head) if part == 0 else head
        w_copies.append(
            pltpu.make_async_copy(
                w_hbm.at[:, pl.ds(pl.multiple_of(col * half, 128), half)],
                w_vmem.at[part], w_sem.at[part],
            )
        )
        w_copies[-1].start()

    posbuf[me] = pos_in[...]
    for g in range(groups):
        kvbuf[z, g, :, rows(s), :] = kv_in[s * groups + g]
        for r in range(rep):
            qbuf[g * rep + r, rows(s), :] = q_in[(s * groups + g) * rep + r]
    m_ref[...] = jnp.full(m_ref.shape, NEG_BIG, jnp.float32)
    acc_ref[...] = jnp.zeros(acc_ref.shape, jnp.float32)

    def own_parts(g):
        for d in (1, 2, 3):
            kv_copy(d, g).wait_recv()
            p = peer(d)
            z_send_part(g, kvbuf.at[z, g, :, rows(p), :], p)

    def compute(layer, g):
        key_pos = jnp.concatenate([posbuf[layer * QUAD + i] for i in range(QUAD)], axis=1)
        key_pos = key_pos.astype(jnp.float32)

        key_row = key_pos
        key_t[...] = kvbuf[layer, g, 0].T
        lanes = key_row.shape[1] // 128
        q_rows = 256
        tiles = tok_z // q_rows

        def wide(a, count):
            return jnp.concatenate([a] * count, axis=1)

        def tile(i, _):
            span = pl.ds(pl.multiple_of(i * q_rows, q_rows), q_rows)
            values = kvbuf[layer, g, 1]
            extended = jnp.concatenate([values, jnp.ones_like(values)], axis=1)
            heads = range(g * rep, (g + 1) * rep)
            old_max = [m_ref[h, span, :] for h in heads]
            old_acc = [acc_ref[h, span, :] for h in heads]
            visible = key_row <= wide(qcol[span, :], lanes)
            raw = [
                jnp.dot(qbuf[h, span, :], key_t[...], preferred_element_type=jnp.float32)
                for h in heads
            ]
            new_max, new_acc = [], []
            for x, m_old, a_old in zip(raw, old_max, old_acc):
                x = jnp.where(visible, x * EXP2_SCALE, NEG_BIG)
                m_new = jnp.maximum(m_old, jnp.max(x, axis=1, keepdims=True))
                decay = jnp.exp2(m_old - m_new)
                weights = jnp.exp2(x - wide(m_new, lanes)).astype(jnp.bfloat16)
                new = jnp.dot(weights, extended, preferred_element_type=jnp.float32)
                new_max.append(m_new)
                new_acc.append(a_old * wide(decay, 2) + new)
            for h, m_new, a_new in zip(heads, new_max, new_acc):
                m_ref[h, span, :] = m_new
                acc_ref[h, span, :] = a_new
            return 0

        lax.fori_loop(0, tiles, tile, 0, unroll=1)

    def att_copy(d, g):
        p = peer(d)
        cols = pl.ds(g * rep * hd, rep * hd)
        return remote(
            obuf.at[rows(p), cols], attbuf.at[s, :, cols],
            att_send.at[d, g], att_recv.at[d, g], z * QUAD + p,
        )

    def finish(g):
        for r in range(rep):
            for t in range(QUAD):
                part = acc_ref[g * rep + r, t * tok:(t + 1) * tok, :]
                done = (part[:, :hd] / part[:, hd:]).astype(jnp.bfloat16)
                obuf[t * tok:(t + 1) * tok, (g * rep + r) * hd:(g * rep + r + 1) * hd] = done
        for d in (3, 2, 1):
            att_copy(d, g).start()
        cols = slice(g * rep * hd, (g + 1) * rep * hd)
        attbuf[s, :, cols] = obuf[rows(s), cols]

    units = [(k, g, up) for k in range(1, nz) for g in range(groups) for up in (False, True)]
    middle = (z > 0) & (z < nz - 1)

    def exists(k, up):
        return z - k >= 0 if up else z + k < nz

    def arrive(i):
        k, g, up = units[i]

        @pl.when(exists(k, up))
        def _():
            if up:
                wait_below(k, g)

                @pl.when(z < nz - 1)
                def _():
                    up_chunk(k, g).start()
            else:
                wait_above(k, g)

                @pl.when(z > 0)
                def _():
                    down_chunk(k, g).start()

    def ahead(i):
        if i < len(units):
            @pl.when(middle)
            def _():
                arrive(i)

    for g in range(groups):
        own_parts(g)
        if g == 0:
            for d in range(1, n_ctx):
                pos_copy(d).wait_recv()
            for i in range(QUAD):
                line = posbuf[z * QUAD + i].astype(jnp.float32)
                for j in range(tok // 128):
                    piece = jnp.broadcast_to(line[:, j * 128:(j + 1) * 128], (128, 128))
                    qcol[i * tok + j * 128:i * tok + (j + 1) * 128, :] = piece.T
        if g == groups - 1:
            ahead(0)
        for d in (1, 2, 3):
            q_copy(d, g).wait_recv()
        compute(z, g)

    for i, (k, g, up) in enumerate(units):
        ahead(i + 1)

        @pl.when(jnp.logical_not(middle))
        def _():
            arrive(i)

        @pl.when(exists(k, up))
        def _():
            compute(z - k if up else z + k, g)

        if k == nz - 1 and up:
            finish(g)
    if nz == 1:
        for g in range(groups):
            finish(g)

    def y_copy(b):
        return remote(
            sendbuf.at[b], recvbuf.at[b], y_send.at[b], y_recv.at[b], me, 1 - head
        )

    for g in range(groups):
        for d in (1, 2, 3):
            att_copy(d, g).wait_recv()

    def product(part, b):
        total = None
        depth = groups * rep * hd
        for j in range(QUAD):
            term = jnp.dot(
                attbuf[j],
                w_vmem[part, j * depth:(j + 1) * depth, b * width:(b + 1) * width],
                preferred_element_type=jnp.float32,
            )
            total = term if total is None else total + term
        return total

    w_copies[0].wait()
    for b in range(n_blocks):
        sendbuf[b] = product(0, b).astype(jnp.bfloat16)
        y_copy(b).start()
    w_copies[1].wait()
    for b in range(n_blocks):
        ownbuf[b] = product(1, b)
    for b in range(n_blocks):
        y_copy(b).wait_recv()
        out_ref[:, b * width:(b + 1) * width] = (
            ownbuf[b] + recvbuf[b].astype(jnp.float32)
        ).astype(jnp.bfloat16)

    for d in range(1, n_ctx):
        pos_copy(d).wait_send()
    for g in range(groups):
        for d in (1, 2, 3):
            kv_copy(d, g).wait_send()
            q_copy(d, g).wait_send()
            att_copy(d, g).wait_send()
        for k in range(nz - 1):
            @pl.when((z > 0) & (z + k < nz))
            def _():
                down_chunk(k, g).wait_send()

            @pl.when((z < nz - 1) & (z - k >= 0))
            def _():
                up_chunk(k, g).wait_send()
    for b in range(n_blocks):
        y_copy(b).wait_send()


def fused_on_device(n_ctx, query_heads, key_heads, value_heads, positions, out_weight):
    tok, n_q, hd = query_heads.shape
    n_kv = key_heads.shape[1]
    q = jnp.transpose(query_heads, (1, 0, 2))
    kv = jnp.transpose(jnp.stack([key_heads, value_heads]), (2, 0, 1, 3))
    pos = positions.reshape(1, tok)
    nz = n_ctx // QUAD
    groups = n_kv // QUAD
    q_dev = n_q // QUAD
    tok_z = QUAD * tok
    rows_w, model = out_weight.shape
    half = model // 2
    n_blocks = 3 if half % 384 == 0 else 1
    width = half // n_blocks
    vmem = pltpu.VMEM
    dma = pltpu.SemaphoreType.DMA
    whole = pl.BlockSpec(memory_space=pltpu.VMEM)
    return pl.pallas_call(
        functools.partial(fused_kernel, n_ctx, n_blocks),
        out_shape=jax.ShapeDtypeStruct((tok, half), jnp.bfloat16),
        in_specs=[whole, whole, whole, pl.BlockSpec(memory_space=pl.ANY)],
        out_specs=whole,
        scratch_shapes=[
            vmem((nz, groups, 2, tok_z, hd), jnp.bfloat16),
            vmem((q_dev, tok_z, hd), jnp.bfloat16),
            vmem((n_ctx, 1, tok), jnp.int32),
            vmem((tok_z, 128), jnp.float32),
            vmem((q_dev, tok_z, hd), jnp.float32),
            vmem((q_dev, tok_z, 2 * hd), jnp.float32),
            vmem((tok_z, q_dev * hd), jnp.bfloat16),
            vmem((QUAD, tok, q_dev * hd), jnp.bfloat16),
            vmem((2, rows_w, half), jnp.bfloat16),
            vmem((n_blocks, tok, width), jnp.bfloat16),
            vmem((n_blocks, tok, width), jnp.bfloat16),
            vmem((n_blocks, tok, width), jnp.float32),
            vmem((hd, tok_z), jnp.bfloat16),
            dma((2,)),
            dma((n_ctx,)), dma((n_ctx,)),
            dma((QUAD, groups)), dma((QUAD, groups)),
            dma((QUAD, groups)), dma((QUAD, groups)),
            dma((nz, groups)), dma((nz, groups)),
            dma((nz + 1, groups)), dma((nz + 1, groups)),
            dma((QUAD, groups)), dma((QUAD, groups)),
            dma((n_blocks,)), dma((n_blocks,)),
        ],
        compiler_params=pltpu.CompilerParams(
            collective_id=0, has_side_effects=True, vmem_limit_bytes=62 * 1024 * 1024
        ),
    )(q, kv, pos, out_weight)


def solution(mesh):
    placed = (
        P("ctx", "head", None),
        P("ctx", "head", None),
        P("ctx", "head", None),
        P("ctx"),
        P("head", None),
    )
    n_ctx, n_head = mesh.shape["ctx"], mesh.shape["head"]

    def on_device(query_heads, key_heads, value_heads, positions, out_weight):
        args = (query_heads, key_heads, value_heads, positions, out_weight)
        fits = (
            n_head == 2 and n_ctx % QUAD == 0 and key_heads.shape[1] % QUAD == 0
            and query_heads.shape[2] == 128 and query_heads.shape[0] % 128 == 0
            and out_weight.shape[1] % 256 == 0
        )
        if fits:
            return fused_on_device(n_ctx, *args)
        return plain_on_device(*args)

    return jax.shard_map(
        on_device, mesh=mesh, in_specs=placed, out_specs=P("ctx", "head"), check_vma=False
    )
```
